32 devices in a mesh: dp: 16 (over z, x, core), tensor: 2 (over y).
Axes of the slice: x: 2, y: 2, z: 4, core: 2. Of those that a mesh axis runs over, the one named last changes fastest.
Arguments:
- residual: bfloat16 [4096, 4096], P('dp', 'tensor'), may hold values from -6 to 6
- fresh_qkv: bfloat16 [4096, 3, 2048], P('dp', None, 'tensor'), may hold values from -110 to 110
- active: int32 [4096], P('dp'), may hold values from 0 to 1
- home_slot: int32 [4096], P('dp'), may hold values from 0 to 4095, as said below
- kv_cache: bfloat16 [4096, 2, 16, 2048], P('dp', None, None, 'tensor'), may hold values from -6 to 6
- lengths: int32 [4096], P('dp'), may hold values from 2 to 16
- w_out: bfloat16 [2048, 4096], P('tensor'), may hold values from -0.125 to 0.125
Outputs:
- updated: bfloat16 [4096, 4096], P('dp', 'tensor')
The draws below stay inside these ranges and needn't reach their ends.
Inputs may be any that keep to these rules, and one draw needn't show every extreme that they name: Each dp group owns the slots 256 * g to 256 * g + 255; home_slot is a permutation. Among the streams of one dp group, at most 16 active streams have slots in the same owning group, and this is reached in every draw.
All inputs are finite; a program needn't handle non-finite values.
Results may differ from the reference program's by a relative error of at most 0.0062.
Values may be sent and summed in bfloat16 or wider, within the bound.
A program may use at most 128 MiB of HBM per device.

```python
import jax
import jax.numpy as jnp
from jax import lax

D = 4096
HEADS = 16
HD = 128
S_DEV = 256
L = 16
CAP = 16
STREAMS = 4096


def routing(key):
    base = jax.random.fold_in(key, 101)
    groups = STREAMS // S_DEV
    stream_index = jnp.arange(STREAMS, dtype=jnp.int32)
    source = stream_index // S_DEV
    within = stream_index % S_DEV
    shuffled = jax.random.permutation(jax.random.fold_in(base, 1), groups).astype(jnp.int32)
    inverse = jnp.argsort(shuffled).astype(jnp.int32)
    values = jnp.arange(groups, dtype=jnp.int32)
    priority = jnp.where(values == 1, 0, jnp.where(values == groups - 1, 1, jnp.where(values == groups // 2, 2, 3 + inverse)))
    offsets = jnp.argsort(priority).astype(jnp.int32)[:S_DEV // CAP]
    owner_group = (source + offsets[within // CAP]) % groups
    ranking = jax.random.randint(jax.random.fold_in(base, 2), (groups, S_DEV), 0, 1 << 20) * S_DEV + jnp.arange(S_DEV, dtype=jnp.int32)[None, :]
    slot_order = jnp.argsort(ranking, axis=1).astype(jnp.int32)
    home_slot = owner_group * S_DEV + slot_order[owner_group, within]
    active_level = jax.random.randint(jax.random.fold_in(base, 3), (groups,), 2, 9)
    dice_roll = jax.random.randint(jax.random.fold_in(base, 4), (STREAMS,), 0, 8)
    active = jnp.logical_or(dice_roll < active_level[owner_group], stream_index < CAP)
    return (home_slot.astype(jnp.int32), active.astype(jnp.int32))


def draw_home_slot(key, part):
    return routing(key)[0]


def draw_active(key, part):
    return routing(key)[1]


def draw_fresh_qkv(key, part):
    drawn = jnp.clip(jax.random.normal(jax.random.fold_in(key, 201), (STREAMS, 3, HEADS * HD), jnp.float32), -6.0, 6.0)
    return drawn.astype(jnp.bfloat16)


def draw_kv_cache(key, part):
    drawn = jnp.clip(jax.random.normal(jax.random.fold_in(key, 202), (STREAMS, 2, L, HEADS * HD), jnp.float32), -6.0, 6.0)
    return drawn.astype(jnp.bfloat16)


def place_ends(array, stream_key, least, top_value):
    longest = array.shape.index(max(array.shape))
    spots = []
    for shift in (0, 1):
        where = [jax.random.randint(jax.random.fold_in(stream_key, axis), (), 0, length) for axis, length in enumerate(array.shape)]
        where[longest] = (where[longest] + shift) % array.shape[longest]
        spots.append(tuple(where))
    return array.at[spots[0]].set(least).at[spots[1]].set(top_value)


def level_of(own_key, shape, shards, least, largest):
    factor_of = 1.0
    for position, shards_of in shards:
        draws = jax.random.uniform(jax.random.fold_in(jax.random.fold_in(own_key, 6), position), (shards_of,), jnp.float32, least / len(shards), largest / len(shards))
        factor_of = factor_of * jnp.repeat(jnp.exp(draws), shape[position] // shards_of).reshape((-1,) + (1,) * (len(shape) - 1 - position))
    return factor_of


def bell_draw(own_key, extent, width, most, split=(), held_as=jnp.bfloat16):
    result = jax.random.normal(own_key, extent, jnp.float32) * width
    if len(split) > 0:
        result = level_of(own_key, extent, split, -0.22, 0.18) * result
    return jnp.clip(result, min=-most, max=most).astype(held_as)


def setup_inputs(seed: int = 0) -> dict:
    keys = jax.random.split(jax.random.key(seed), 8)
    return {
        "residual": bell_draw(keys[0], (STREAMS, D), 1.0, 6.0, ((0, 16), (1, 2))),
        "fresh_qkv": draw_fresh_qkv(jax.random.fold_in(keys[7], 71), 0),
        "active": draw_active(jax.random.fold_in(keys[7], 71), 0),
        "home_slot": draw_home_slot(jax.random.fold_in(keys[7], 71), 0),
        "kv_cache": draw_kv_cache(jax.random.fold_in(keys[7], 71), 0),
        "lengths": place_ends(jax.random.randint(keys[5], (STREAMS,), 2, L + 1), jax.random.fold_in(keys[5], 1), 2, L).astype(jnp.int32),
        "w_out": bell_draw(keys[6], (HEADS * HD, D), (HEADS * HD) ** -0.5, 0.125, ((0, 2),)),
    }


def attend(query, key_rows, value_rows, key_new, value_new, length):
    score_scale = HD ** -0.5
    scores = jnp.einsum("bhd,blhd->bhl", query.astype(jnp.float32), key_rows.astype(jnp.float32)) * score_scale
    positions = jnp.arange(L, dtype=jnp.int32)
    in_cache = positions[None, None, :] < length[:, None, None]
    scores = jnp.where(in_cache, scores, jnp.float32(-1e30))
    own_score = jnp.sum(query.astype(jnp.float32) * key_new.astype(jnp.float32), axis=-1) * score_scale
    row_max = jnp.maximum(jnp.max(scores, axis=-1), own_score)
    weights_raw = jnp.exp(scores - row_max[..., None])
    own_raw = jnp.exp(own_score - row_max)
    denominator = jnp.sum(weights_raw, axis=-1) + own_raw
    weights = (weights_raw / denominator[..., None]).astype(jnp.bfloat16)
    own_weight = (own_raw / denominator).astype(jnp.bfloat16)
    mixed = jnp.einsum("bhl,blhd->bhd", weights.astype(jnp.float32), value_rows.astype(jnp.float32))
    mixed = mixed + own_weight.astype(jnp.float32)[..., None] * value_new.astype(jnp.float32)
    return mixed.astype(jnp.bfloat16).reshape(query.shape[0], -1)


def reference(residual, fresh_qkv, active, home_slot, kv_cache, lengths, w_out):
    groups = STREAMS // S_DEV

    def one_group(group):
        start = (group * S_DEV).astype(jnp.int32)
        streams = start + jnp.arange(S_DEV, dtype=jnp.int32)
        slots = home_slot[streams]
        fresh_rows = jnp.take(fresh_qkv, streams, axis=0).reshape(S_DEV, 3, HEADS, HD)
        cache_rows = jnp.take(kv_cache, slots, axis=0).reshape(S_DEV, 2, L, HEADS, HD)
        attended = attend(fresh_rows[:, 0], cache_rows[:, 0], cache_rows[:, 1], fresh_rows[:, 1], fresh_rows[:, 2], lengths[slots])
        projected = jnp.dot(attended, w_out, preferred_element_type=jnp.float32)
        rows = lax.dynamic_slice_in_dim(residual, start, S_DEV, 0).astype(jnp.float32)
        flags = active[streams].astype(jnp.float32)
        return (rows + flags[:, None] * projected).astype(jnp.bfloat16)

    updated = lax.map(one_group, jnp.arange(groups, dtype=jnp.int32))
    return updated.reshape(STREAMS, D)
```

```python
import functools

import jax
import jax.numpy as jnp
from jax import lax
from jax.experimental import pallas as pl
from jax.experimental.pallas import tpu as pltpu
from jax.sharding import PartitionSpec as P

HD = 128


def attend_local(fresh_rows, kv_cache, lengths, heads_local):
    streams_here = fresh_rows.shape[0]
    cache_len = kv_cache.shape[2]
    head_size = fresh_rows.shape[1] // (3 * heads_local)
    score_scale = head_size ** (-0.5)
    fresh_split = fresh_rows.reshape(streams_here, 3, heads_local, head_size)
    query = fresh_split[:, 0]
    key_rows = kv_cache[:, 0].reshape(streams_here, cache_len, heads_local, head_size)
    value_rows = kv_cache[:, 1].reshape(streams_here, cache_len, heads_local, head_size)
    scores = (
        jnp.einsum("bhd,blhd->bhl", query, key_rows, preferred_element_type=jnp.float32)
        * score_scale
    )
    positions = jnp.arange(cache_len, dtype=jnp.int32)
    in_cache = positions[None, None, :] < lengths[:, None, None]
    scores = jnp.where(in_cache, scores, jnp.float32(-1e30))
    own_score = (
        jnp.sum(query.astype(jnp.float32) * fresh_split[:, 1].astype(jnp.float32), axis=-1)
        * score_scale
    )
    row_max = jnp.maximum(jnp.max(scores, axis=-1), own_score)
    weights_raw = jnp.exp(scores - row_max[..., None])
    own_raw = jnp.exp(own_score - row_max)
    denominator = jnp.sum(weights_raw, axis=-1) + own_raw
    weights = (weights_raw / denominator[..., None]).astype(jnp.bfloat16)
    own_weight = (own_raw / denominator).astype(jnp.bfloat16)
    mixed = jnp.einsum("bhl,blhd->bhd", weights, value_rows, preferred_element_type=jnp.float32)
    mixed = mixed + own_weight.astype(jnp.float32)[..., None] * fresh_split[:, 2].astype(
        jnp.float32
    )
    return mixed.astype(jnp.bfloat16).reshape(streams_here, heads_local * head_size)


def general_body(residual, fresh_qkv, active, home_slot, kv_cache, lengths, w_out):
    groups = lax.axis_size("dp")
    group_here = lax.axis_index("dp")
    streams_here = home_slot.shape[0]
    width_here = fresh_qkv.shape[2]
    heads_local = width_here // HD
    capacity = max(2, streams_here // groups)
    slot_count = groups * capacity
    owner_group = home_slot // streams_here
    is_active = active > 0
    earlier = jnp.arange(streams_here)[:, None] < jnp.arange(streams_here)[None, :]
    same_owner = (
        (owner_group[:, None] == owner_group[None, :])
        & is_active[:, None]
        & is_active[None, :]
        & earlier
    )
    send_rank = jnp.sum(same_owner.astype(jnp.int32), axis=0)
    target = owner_group * capacity + send_rank
    placed = (jnp.arange(slot_count, dtype=jnp.int32)[:, None] == target[None, :]) & is_active[
        None, :
    ]
    placing = placed.astype(jnp.bfloat16)
    fresh_flat = fresh_qkv.reshape(streams_here, 3 * width_here)
    send_rows = jnp.dot(placing, fresh_flat, preferred_element_type=jnp.float32).astype(
        jnp.bfloat16
    )
    send_rows = send_rows.reshape(groups, capacity, 3 * width_here)
    slot_ids = jnp.sum(jnp.where(placed, home_slot[None, :] + 1, 0), axis=1) - 1
    slot_ids = slot_ids.reshape(groups, capacity)
    got_rows, got_ids = (
        lax.all_to_all(send_rows, "dp", split_axis=0, concat_axis=0, tiled=True),
        lax.all_to_all(slot_ids, "dp", split_axis=0, concat_axis=0, tiled=True),
    )
    local_slot = got_ids.reshape(slot_count) - group_here * streams_here
    matched = (local_slot[None, :] == jnp.arange(streams_here, dtype=jnp.int32)[:, None]).astype(
        jnp.bfloat16
    )
    owned = jnp.dot(
        matched, got_rows.reshape(slot_count, 3 * width_here), preferred_element_type=jnp.float32
    ).astype(jnp.bfloat16)
    attended = attend_local(owned, kv_cache, lengths, heads_local)
    heads_rows = jnp.dot(matched.T, attended, preferred_element_type=jnp.float32).astype(
        jnp.bfloat16
    )
    returned = lax.all_to_all(
        heads_rows.reshape(groups, capacity, width_here),
        "dp",
        split_axis=0,
        concat_axis=0,
        tiled=True,
    )
    source_rows = jnp.dot(
        placing.T, returned.reshape(slot_count, width_here), preferred_element_type=jnp.float32
    ).astype(jnp.bfloat16)
    partial_rows = jnp.dot(source_rows, w_out, preferred_element_type=jnp.float32)
    gained = lax.psum_scatter(partial_rows, "tensor", scatter_dimension=1, tiled=True)
    return (residual.astype(jnp.float32) + gained).astype(jnp.bfloat16)


MESH = pl.DeviceIdType.MESH
F32 = jnp.float32
BF16 = jnp.bfloat16
LANES = 128
KV_PARTS = 4
COLUMN_CHUNKS = 4


def column_of(row, width):
    return jnp.transpose(jnp.broadcast_to(row, (width, row.shape[1])))


def iota(shape, dim):
    return lax.broadcasted_iota(jnp.int32, shape, dim)


def kernel(
    n, heads, home_ref, active_ref, lengths_ref, fresh_ref, kv_hbm, w_hbm, residual_hbm,
    out_ref,
    kv, w, residual, send_q, got_q, send_a, got_a, owned, own, length_col, placing_t, mixed,
    attended, part_send, part_got, kept,
    kv_sem, w_sem, residual_sem, q_send_sem, q_got_sem, a_send_sem, a_got_sem, p_send_sem,
    p_got_sem,
):
    me = lax.axis_index("dp")
    side = lax.axis_index("tensor")
    other = 1 - side
    streams = home_ref.shape[1]
    width = heads * HD
    capacity = send_q.shape[1]
    cache_len = kv.shape[2]
    scale = HD ** -0.5
    order = sorted(range(1, n), key=lambda k: abs(n - 2 * k))

    barrier = pltpu.get_barrier_semaphore()
    for k in order:
        pl.semaphore_signal(
            barrier, inc=1, device_id={"dp": lax.rem(me + k, n)}, device_id_type=MESH
        )
    pl.semaphore_signal(barrier, inc=1, device_id={"tensor": other}, device_id_type=MESH)

    part = streams // KV_PARTS
    kv_copies = [
        pltpu.make_async_copy(
            kv_hbm.at[pl.ds(i * part, part)], kv.at[pl.ds(i * part, part)], kv_sem.at[i]
        )
        for i in range(KV_PARTS)
    ]
    for copy in kv_copies:
        copy.start()
    w_copy = pltpu.make_async_copy(w_hbm, w, w_sem)
    w_copy.start()
    residual_copy = pltpu.make_async_copy(residual_hbm, residual, residual_sem)
    residual_copy.start()

    home = home_ref[...]
    is_active = active_ref[...] > 0
    shift = streams.bit_length() - 1
    owner = jnp.where(is_active, lax.shift_right_logical(home, shift), -1).astype(F32)
    local = ((home & (streams - 1)) + 1).astype(F32)
    square = (streams, streams)
    owner_cols = jnp.broadcast_to(owner, square)
    same = (
        (owner_cols == jnp.transpose(owner_cols))
        & (owner_cols >= 0)
        & (iota(square, 0) < iota(square, 1))
    )
    rank = jnp.sum(jnp.where(same, 1.0, 0.0), axis=0, keepdims=True)
    target = jnp.where(owner >= 0, owner * capacity + rank, -1.0)
    placing = jnp.where(iota(square, 0).astype(F32) == target, 1.0, 0.0)
    placed = placing.astype(BF16)
    ids = column_of(local, LANES).astype(BF16)
    rows = jnp.dot(placed, fresh_ref[:, :width], preferred_element_type=F32).astype(BF16)
    send_q[:, :, :width] = rows.reshape(n, capacity, width)
    rows = jnp.dot(placed, ids, preferred_element_type=F32).astype(BF16)
    send_q[:, :, width:] = rows.reshape(n, capacity, LANES)
    placing_t[...] = jnp.transpose(placing).astype(BF16)
    length_col[...] = column_of(lengths_ref[...].astype(F32), LANES)

    pl.semaphore_wait(barrier, n)

    def exchange(source, landing, send_sem, got_sem):
        copies = []
        for k in order:
            peer = lax.rem(me + k, n)
            copies.append(
                pltpu.make_async_remote_copy(
                    src_ref=source.at[peer],
                    dst_ref=landing.at[me],
                    send_sem=send_sem.at[k],
                    recv_sem=got_sem.at[k],
                    device_id={"dp": peer},
                    device_id_type=MESH,
                )
            )
        for copy in copies:
            copy.start()
        return copies

    copies = exchange(send_q, got_q, q_send_sem, q_got_sem)
    own_block = pltpu.make_async_copy(send_q.at[me], got_q.at[me], q_got_sem.at[0])
    own_block.start()
    lane = iota((streams, LANES), 1)
    own_scores = jnp.zeros((streams, LANES), F32)
    for h in range(heads):
        query = fresh_ref[:, h * HD : (h + 1) * HD].astype(F32)
        key = fresh_ref[:, width + h * HD : width + (h + 1) * HD].astype(F32)
        own_h = jnp.sum(query * key, axis=1, keepdims=True) * scale
        own_scores = jnp.where(lane == h, own_h, own_scores)
    own[...] = own_scores
    own_block.wait()
    for copy in copies:
        copy.wait()

    got_ids = got_q[:, :, width:].reshape(n * capacity, LANES)[:, :1].astype(F32) - 1.0
    matched_t = jnp.where(iota(square, 1).astype(F32) == got_ids, 1.0, 0.0)
    matched = jnp.transpose(matched_t).astype(BF16)
    owned[...] = jnp.dot(
        matched, got_q[:, :, :width].reshape(n * capacity, width), preferred_element_type=F32
    ).astype(BF16)
    matched_t = matched_t.astype(BF16)
    for copy in kv_copies:
        copy.wait()

    batch = 16
    spread = (batch, batch * cache_len)
    in_slot = iota(spread, 1) // cache_len == iota(spread, 0)
    position = lax.rem(iota(spread, 1), cache_len).astype(F32)
    small_lane = iota((batch, LANES), 1)

    def attend(step, carry):
        slots = pl.ds(pl.multiple_of(step * batch, batch), batch)
        queries = owned[slots, :]
        valid = in_slot & (position < length_col[slots, :1])
        sums = jnp.zeros((batch, LANES), F32)
        for h in range(heads):
            span = slice(h * HD, (h + 1) * HD)
            keys = kv[slots, 0, :, span].reshape(batch * cache_len, HD)
            values = kv[slots, 1, :, span].reshape(batch * cache_len, HD)
            scores = (
                lax.dot_general(
                    queries[:, span], keys, (((1,), (1,)), ((), ())), preferred_element_type=F32
                )
                * scale
            )
            scores = jnp.where(valid, scores, -1e30)
            top = jnp.max(scores, axis=1, keepdims=True)
            raw = jnp.exp(scores - top)
            total = jnp.sum(raw, axis=1, keepdims=True)
            weights = (raw / total).astype(BF16)
            mixed[slots, span] = jnp.dot(weights, values, preferred_element_type=F32).astype(BF16)
            here = (lax.rem(small_lane, heads) == h) & (small_lane < 3 * heads)
            sums = jnp.where(here, top + jnp.log(total), sums)
        first = sums.astype(BF16).astype(F32)
        second = (sums - first).astype(BF16).astype(F32)
        third = sums - first - second
        digits = jnp.where(
            small_lane < heads, first, jnp.where(small_lane < 2 * heads, second, third)
        )
        digits = jnp.where(small_lane == 3 * heads, 1.0, digits)
        mixed[slots, width:] = digits.astype(BF16)
        return carry

    lax.fori_loop(0, streams // batch, attend, 0)

    back = jnp.dot(matched_t, mixed[...], preferred_element_type=F32).astype(BF16)
    send_a[...] = back.reshape(n, capacity, width + LANES)
    copies = exchange(send_a, got_a, a_send_sem, a_got_sem)
    own_block = pltpu.make_async_copy(send_a.at[me], got_a.at[me], a_got_sem.at[0])
    own_block.start()
    w_copy.wait()
    residual_copy.wait()
    own_block.wait()
    for copy in copies:
        copy.wait()

    place_back = placing_t[...]
    extra = jnp.dot(
        place_back,
        got_a[:, :, width:].reshape(n * capacity, LANES),
        preferred_element_type=F32,
    )
    flag = extra[:, 3 * heads : 3 * heads + 1]
    own_scores = own[...]
    for h in range(heads):
        span = slice(h * HD, (h + 1) * HD)
        cached = jnp.dot(
            place_back,
            got_a[:, :, span].reshape(n * capacity, HD),
            preferred_element_type=F32,
        )
        lse = (
            extra[:, h : h + 1]
            + extra[:, heads + h : heads + h + 1]
            + extra[:, 2 * heads + h : 2 * heads + h + 1]
        )
        own_h = own_scores[:, h : h + 1]
        top = jnp.maximum(lse, own_h)
        from_cache = jnp.exp(lse - top)
        from_own = jnp.exp(own_h - top)
        share = flag / (from_cache + from_own)
        value = fresh_ref[:, 2 * width + h * HD : 2 * width + (h + 1) * HD].astype(F32)
        attended[:, span] = (
            (from_cache * share) * cached + (from_own * share) * value
        ).astype(BF16)

    columns = residual.shape[1]
    chunk = columns // COLUMN_CHUNKS
    sends = []
    for c in range(COLUMN_CHUNKS):
        span = pl.ds(pl.multiple_of(other * columns + c * chunk, LANES), chunk)
        part_send[c] = jnp.dot(
            attended[...], w[:, span], preferred_element_type=F32
        ).astype(BF16)
        copy = pltpu.make_async_remote_copy(
            src_ref=part_send.at[c],
            dst_ref=part_got.at[c],
            send_sem=p_send_sem.at[c],
            recv_sem=p_got_sem.at[c],
            device_id={"tensor": other},
            device_id_type=MESH,
        )
        copy.start()
        sends.append(copy)
    for c in range(COLUMN_CHUNKS):
        span = pl.ds(pl.multiple_of(side * columns + c * chunk, LANES), chunk)
        kept[c] = residual[:, c * chunk : (c + 1) * chunk].astype(F32) + jnp.dot(
            attended[...], w[:, span], preferred_element_type=F32
        )
    for c in range(COLUMN_CHUNKS):
        sends[c].wait()
        out_ref[:, c * chunk : (c + 1) * chunk] = (
            kept[c] + part_got[c].astype(F32)
        ).astype(BF16)


def fused_body(residual, fresh_qkv, active, home_slot, kv_cache, lengths, w_out):
    n = lax.axis_size("dp")
    streams, columns = residual.shape
    width = fresh_qkv.shape[2]
    heads = width // HD
    capacity = streams // n
    row = (n, capacity, width + LANES)
    chunk = columns // COLUMN_CHUNKS
    vmem = pl.BlockSpec(memory_space=pltpu.VMEM)
    anywhere = pl.BlockSpec(memory_space=pl.ANY)
    dma = pltpu.SemaphoreType.DMA
    return pl.pallas_call(
        functools.partial(kernel, n, heads),
        out_shape=jax.ShapeDtypeStruct((streams, columns), BF16),
        in_specs=[vmem] * 4 + [anywhere] * 3,
        out_specs=vmem,
        scratch_shapes=[
            pltpu.VMEM(kv_cache.shape, BF16),
            pltpu.VMEM(w_out.shape, BF16),
            pltpu.VMEM(residual.shape, BF16),
            pltpu.VMEM(row, BF16),
            pltpu.VMEM(row, BF16),
            pltpu.VMEM(row, BF16),
            pltpu.VMEM(row, BF16),
            pltpu.VMEM((streams, width), BF16),
            pltpu.VMEM((streams, LANES), F32),
            pltpu.VMEM((streams, LANES), F32),
            pltpu.VMEM((streams, streams), BF16),
            pltpu.VMEM((streams, width + LANES), BF16),
            pltpu.VMEM((streams, width), BF16),
            pltpu.VMEM((COLUMN_CHUNKS, streams, chunk), BF16),
            pltpu.VMEM((COLUMN_CHUNKS, streams, chunk), BF16),
            pltpu.VMEM((COLUMN_CHUNKS, streams, chunk), F32),
            dma((KV_PARTS,)),
            dma,
            dma,
            dma((n,)),
            dma((n,)),
            dma((n,)),
            dma((n,)),
            dma((COLUMN_CHUNKS,)),
            dma((COLUMN_CHUNKS,)),
        ],
        compiler_params=pltpu.CompilerParams(
            collective_id=0, has_side_effects=True, vmem_limit_bytes=60 * 1024 * 1024
        ),
    )(
        home_slot.reshape(1, streams),
        active.reshape(1, streams),
        lengths.reshape(1, streams),
        fresh_qkv.reshape(streams, 3 * width),
        kv_cache,
        w_out,
        residual,
    )


def body(residual, fresh_qkv, active, home_slot, kv_cache, lengths, w_out):
    n = lax.axis_size("dp")
    streams = home_slot.shape[0]
    fits = (
        lax.axis_size("tensor") == 2
        and streams % n == 0
        and (streams // n) % 16 == 0
        and streams <= 256
        and streams & (streams - 1) == 0
    )
    chosen = fused_body if fits else general_body
    return chosen(residual, fresh_qkv, active, home_slot, kv_cache, lengths, w_out)


def solution(mesh):
    placed = (
        P("dp", "tensor"),
        P("dp", None, "tensor"),
        P("dp"),
        P("dp"),
        P("dp", None, None, "tensor"),
        P("dp"),
        P("tensor", None),
    )
    return jax.shard_map(
        body, mesh=mesh, in_specs=placed, out_specs=P("dp", "tensor"), check_vma=False
    )
```

```python
import functools

import jax
import jax.numpy as jnp
from jax import lax
from jax.experimental import pallas as pl
from jax.experimental.pallas import tpu as pltpu
from jax.sharding import PartitionSpec as P

HD = 128


def attend_local(fresh_rows, kv_cache, lengths, heads_local):
    streams_here = fresh_rows.shape[0]
    cache_len = kv_cache.shape[2]
    head_size = fresh_rows.shape[1] // (3 * heads_local)
    score_scale = head_size ** (-0.5)
    fresh_split = fresh_rows.reshape(streams_here, 3, heads_local, head_size)
    query = fresh_split[:, 0]
    key_rows = kv_cache[:, 0].reshape(streams_here, cache_len, heads_local, head_size)
    value_rows = kv_cache[:, 1].reshape(streams_here, cache_len, heads_local, head_size)
    scores = (
        jnp.einsum("bhd,blhd->bhl", query, key_rows, preferred_element_type=jnp.float32)
        * score_scale
    )
    positions = jnp.arange(cache_len, dtype=jnp.int32)
    in_cache = positions[None, None, :] < lengths[:, None, None]
    scores = jnp.where(in_cache, scores, jnp.float32(-1e30))
    own_score = (
        jnp.sum(query.astype(jnp.float32) * fresh_split[:, 1].astype(jnp.float32), axis=-1)
        * score_scale
    )
    row_max = jnp.maximum(jnp.max(scores, axis=-1), own_score)
    weights_raw = jnp.exp(scores - row_max[..., None])
    own_raw = jnp.exp(own_score - row_max)
    denominator = jnp.sum(weights_raw, axis=-1) + own_raw
    weights = (weights_raw / denominator[..., None]).astype(jnp.bfloat16)
    own_weight = (own_raw / denominator).astype(jnp.bfloat16)
    mixed = jnp.einsum("bhl,blhd->bhd", weights, value_rows, preferred_element_type=jnp.float32)
    mixed = mixed + own_weight.astype(jnp.float32)[..., None] * fresh_split[:, 2].astype(
        jnp.float32
    )
    return mixed.astype(jnp.bfloat16).reshape(streams_here, heads_local * head_size)


def general_body(residual, fresh_qkv, active, home_slot, kv_cache, lengths, w_out):
    groups = lax.axis_size("dp")
    group_here = lax.axis_index("dp")
    streams_here = home_slot.shape[0]
    width_here = fresh_qkv.shape[2]
    heads_local = width_here // HD
    capacity = max(2, streams_here // groups)
    slot_count = groups * capacity
    owner_group = home_slot // streams_here
    is_active = active > 0
    earlier = jnp.arange(streams_here)[:, None] < jnp.arange(streams_here)[None, :]
    same_owner = (
        (owner_group[:, None] == owner_group[None, :])
        & is_active[:, None]
        & is_active[None, :]
        & earlier
    )
    send_rank = jnp.sum(same_owner.astype(jnp.int32), axis=0)
    target = owner_group * capacity + send_rank
    placed = (jnp.arange(slot_count, dtype=jnp.int32)[:, None] == target[None, :]) & is_active[
        None, :
    ]
    placing = placed.astype(jnp.bfloat16)
    fresh_flat = fresh_qkv.reshape(streams_here, 3 * width_here)
    send_rows = jnp.dot(placing, fresh_flat, preferred_element_type=jnp.float32).astype(
        jnp.bfloat16
    )
    send_rows = send_rows.reshape(groups, capacity, 3 * width_here)
    slot_ids = jnp.sum(jnp.where(placed, home_slot[None, :] + 1, 0), axis=1) - 1
    slot_ids = slot_ids.reshape(groups, capacity)
    got_rows, got_ids = (
        lax.all_to_all(send_rows, "dp", split_axis=0, concat_axis=0, tiled=True),
        lax.all_to_all(slot_ids, "dp", split_axis=0, concat_axis=0, tiled=True),
    )
    local_slot = got_ids.reshape(slot_count) - group_here * streams_here
    matched = (local_slot[None, :] == jnp.arange(streams_here, dtype=jnp.int32)[:, None]).astype(
        jnp.bfloat16
    )
    owned = jnp.dot(
        matched, got_rows.reshape(slot_count, 3 * width_here), preferred_element_type=jnp.float32
    ).astype(jnp.bfloat16)
    attended = attend_local(owned, kv_cache, lengths, heads_local)
    heads_rows = jnp.dot(matched.T, attended, preferred_element_type=jnp.float32).astype(
        jnp.bfloat16
    )
    returned = lax.all_to_all(
        heads_rows.reshape(groups, capacity, width_here),
        "dp",
        split_axis=0,
        concat_axis=0,
        tiled=True,
    )
    source_rows = jnp.dot(
        placing.T, returned.reshape(slot_count, width_here), preferred_element_type=jnp.float32
    ).astype(jnp.bfloat16)
    partial_rows = jnp.dot(source_rows, w_out, preferred_element_type=jnp.float32)
    gained = lax.psum_scatter(partial_rows, "tensor", scatter_dimension=1, tiled=True)
    return (residual.astype(jnp.float32) + gained).astype(jnp.bfloat16)


MESH = pl.DeviceIdType.MESH
F32 = jnp.float32
BF16 = jnp.bfloat16
LANES = 128
KV_PARTS = 4
COLUMN_CHUNKS = 4
ROW_GROUPS = 4
GROUP_ORDER = (0, 2, 1, 3)


def column_of(row, width):
    return jnp.transpose(jnp.broadcast_to(row, (width, row.shape[1])))


def partner_of(me, k, n):
    peer = me
    for bit in range(n.bit_length() - 1):
        if k >> bit & 1:
            peer = peer + (1 - 2 * lax.rem(me // (1 << bit), 2)) * (1 << bit)
    return peer


def iota(shape, dim):
    return lax.broadcasted_iota(jnp.int32, shape, dim)


def kernel(
    n, heads, home_ref, active_ref, lengths_ref, fresh_ref, kv_hbm, w_hbm, residual_hbm,
    out_ref,
    kv, w, residual, send_q, got_q, send_a, got_a, owned, own, length_col, placing_t, mixed,
    key_rows, value_rows, attended, part_send, part_got, kept, gained,
    kv_sem, w_sem, residual_sem, q_send_sem, q_got_sem, a_send_sem, a_got_sem, p_send_sem,
    p_got_sem,
):
    me = lax.axis_index("dp")
    side = lax.axis_index("tensor")
    other = 1 - side
    streams = home_ref.shape[1]
    width = heads * HD
    capacity = send_q.shape[1]
    cache_len = kv.shape[2]
    scale = HD ** -0.5
    order = list(range(n // 2, n)) + list(range(n // 4, n // 2)) + list(range(1, n // 4))
    peers = [partner_of(me, k, n) for k in range(n)]

    barrier = pltpu.get_barrier_semaphore()
    for k in order:
        pl.semaphore_signal(
            barrier, inc=1, device_id={"dp": peers[k]}, device_id_type=MESH
        )
    pl.semaphore_signal(barrier, inc=1, device_id={"tensor": other}, device_id_type=MESH)

    part = streams // KV_PARTS
    kv_copies = [
        pltpu.make_async_copy(
            kv_hbm.at[pl.ds(i * part, part)], kv.at[pl.ds(i * part, part)], kv_sem.at[i]
        )
        for i in range(KV_PARTS)
    ]
    for copy in kv_copies:
        copy.start()
    w_copy = pltpu.make_async_copy(w_hbm, w, w_sem)
    w_copy.start()
    residual_copy = pltpu.make_async_copy(residual_hbm, residual, residual_sem)
    residual_copy.start()

    home = home_ref[...]
    is_active = active_ref[...] > 0
    shift = streams.bit_length() - 1
    owner = jnp.where(is_active, lax.shift_right_logical(home, shift), -1).astype(F32)
    local = ((home & (streams - 1)) + 1).astype(F32)
    square = (streams, streams)
    owner_cols = jnp.broadcast_to(owner, square)
    same = (
        (owner_cols == jnp.transpose(owner_cols))
        & (owner_cols >= 0)
        & (iota(square, 0) < iota(square, 1))
    )
    rank = jnp.sum(jnp.where(same, 1.0, 0.0), axis=0, keepdims=True)
    target = jnp.where(owner >= 0, owner * capacity + rank, -1.0)
    placing = jnp.where(iota(square, 0).astype(F32) == target, 1.0, 0.0)
    placed = placing.astype(BF16)
    ids = column_of(local, LANES).astype(BF16)
    rows = jnp.dot(placed, fresh_ref[:, :width], preferred_element_type=F32).astype(BF16)
    send_q[:, :, :width] = rows.reshape(n, capacity, width)
    rows = jnp.dot(placed, ids, preferred_element_type=F32).astype(BF16)
    send_q[:, :, width:] = rows.reshape(n, capacity, LANES)
    placing_t[...] = jnp.transpose(placing).astype(BF16)
    length_col[...] = column_of(lengths_ref[...].astype(F32), LANES)

    pl.semaphore_wait(barrier, n)

    def exchange(source, landing, send_sem, got_sem):
        copies = [pltpu.make_async_copy(source.at[me], landing.at[me], got_sem.at[0])]
        copies[0].start()
        by_order = {}
        for k in order:
            by_order[k] = pltpu.make_async_remote_copy(
                src_ref=source.at[peers[k]],
                dst_ref=landing.at[me],
                send_sem=send_sem.at[k],
                recv_sem=got_sem.at[k],
                device_id={"dp": peers[k]},
                device_id_type=MESH,
            )
            by_order[k].start()
        return copies + [by_order[k] for k in range(1, n)]

    copies = exchange(send_q, got_q, q_send_sem, q_got_sem)
    key_rows[...] = jnp.dot(
        placed, fresh_ref[:, width : 2 * width], preferred_element_type=F32
    ).astype(BF16)
    value_rows[...] = (
        jnp.dot(placed, fresh_ref[:, 2 * width :], preferred_element_type=F32)
        .astype(BF16)
        .reshape(n, capacity, width)
    )
    lane = iota((streams, LANES), 1)
    own_scores = jnp.zeros((streams, LANES), F32)
    for h in range(heads):
        span = slice(h * HD, (h + 1) * HD)
        query = send_q[:, :, span].reshape(streams, HD).astype(F32)
        key = key_rows[:, span].astype(F32)
        own_h = jnp.sum(query * key, axis=1, keepdims=True) * scale
        own_scores = jnp.where(lane == h, own_h, own_scores)
    own[...] = own_scores.reshape(n, capacity, LANES)
    for copy in copies:
        copy.wait()

    got_ids = got_q[:, :, width:].reshape(n * capacity, LANES)[:, :1].astype(F32) - 1.0
    matched_t = jnp.where(iota(square, 1).astype(F32) == got_ids, 1.0, 0.0)
    matched = jnp.transpose(matched_t).astype(BF16)
    owned[...] = jnp.dot(
        matched, got_q[:, :, :width].reshape(n * capacity, width), preferred_element_type=F32
    ).astype(BF16)
    matched_t = matched_t.astype(BF16)
    for copy in kv_copies:
        copy.wait()

    batch = 16
    spread = (heads * batch, batch * cache_len)
    in_slot = iota(spread, 1) // cache_len == lax.rem(iota(spread, 0), batch)
    position = lax.rem(iota(spread, 1), cache_len).astype(F32)
    small_lane = iota((batch, LANES), 1)

    def attend(step, carry):
        slots = pl.ds(pl.multiple_of(step * batch, batch), batch)
        spans = [slice(h * HD, (h + 1) * HD) for h in range(heads)]
        lens = jnp.concatenate([length_col[slots, :]] * heads, axis=0)[:, :1]
        valid = in_slot & (position < lens)
        scores = jnp.concatenate(
            [
                lax.dot_general(
                    owned[slots, span],
                    kv[slots, 0, :, span].reshape(batch * cache_len, HD),
                    (((1,), (1,)), ((), ())),
                    preferred_element_type=F32,
                )
                for span in spans
            ],
            axis=0,
        )
        scores = jnp.where(valid, scores * scale, -1e30)
        top = jnp.max(scores, axis=1, keepdims=True)
        raw = jnp.exp(scores - top)
        total = jnp.sum(raw, axis=1, keepdims=True)
        weights = (raw / total).astype(BF16)
        lse = top + jnp.log(total)
        sums = jnp.zeros((batch, LANES), F32)
        for h, span in enumerate(spans):
            rows = slice(h * batch, (h + 1) * batch)
            mixed[slots, span] = jnp.dot(
                weights[rows],
                kv[slots, 1, :, span].reshape(batch * cache_len, HD),
                preferred_element_type=F32,
            ).astype(BF16)
            here = (lax.rem(small_lane, heads) == h) & (small_lane < 3 * heads)
            sums = jnp.where(here, lse[rows], sums)
        first = sums.astype(BF16).astype(F32)
        second = (sums - first).astype(BF16).astype(F32)
        third = sums - first - second
        digits = jnp.where(
            small_lane < heads, first, jnp.where(small_lane < 2 * heads, second, third)
        )
        mixed[slots, width:] = digits.astype(BF16)
        return carry

    lax.fori_loop(0, streams // batch, attend, 0)

    back = jnp.dot(matched_t, mixed[...], preferred_element_type=F32).astype(BF16)
    send_a[...] = back.reshape(n, capacity, width + LANES)
    copies = exchange(send_a, got_a, a_send_sem, a_got_sem)
    w_copy.wait()
    residual_copy.wait()

    columns = residual.shape[1]
    step = columns // COLUMN_CHUNKS
    members = n // ROW_GROUPS
    sends = []
    for g, first_k in enumerate(GROUP_ORDER):
        group = range(first_k * members, (first_k + 1) * members)
        for k in group:
            if k:
                copies[k].wait_recv()
            else:
                copies[k].wait()
        arrived = jnp.concatenate([got_a[peers[k]] for k in group], axis=0).astype(F32)
        own_rows = jnp.concatenate([own[peers[k]] for k in group], axis=0)
        values = jnp.concatenate([value_rows[peers[k]] for k in group], axis=0).astype(F32)
        for h in range(heads):
            span = slice(h * HD, (h + 1) * HD)
            at = width + h
            lse = (
                arrived[:, at : at + 1]
                + arrived[:, at + heads : at + heads + 1]
                + arrived[:, at + 2 * heads : at + 2 * heads + 1]
            )
            own_h = own_rows[:, h : h + 1]
            top = jnp.maximum(lse, own_h)
            from_cache = jnp.exp(lse - top)
            from_own = jnp.exp(own_h - top)
            share = 1.0 / (from_cache + from_own)
            attended[g, :, span] = (
                (from_cache * share) * arrived[:, span] + (from_own * share) * values[:, span]
            ).astype(BF16)
        for c in range(COLUMN_CHUNKS):
            here = pl.ds(pl.multiple_of(other * columns + c * step, LANES), step)
            part_send[g, :, c * step : (c + 1) * step] = jnp.dot(
                attended[g], w[:, here], preferred_element_type=F32
            ).astype(BF16)
        copy = pltpu.make_async_remote_copy(
            src_ref=part_send.at[g],
            dst_ref=part_got.at[g],
            send_sem=p_send_sem.at[g],
            recv_sem=p_got_sem.at[g],
            device_id={"tensor": other},
            device_id_type=MESH,
        )
        copy.start()
        sends.append(copy)
        for c in range(COLUMN_CHUNKS):
            here = pl.ds(pl.multiple_of(side * columns + c * step, LANES), step)
            kept[g, :, c * step : (c + 1) * step] = jnp.dot(
                attended[g], w[:, here], preferred_element_type=F32
            )
    for k in range(1, n):
        copies[k].wait_send()
    for g, first_k in enumerate(GROUP_ORDER):
        sends[g].wait()
        total = kept[g] + part_got[g].astype(F32)
        high = total.astype(BF16)
        low = (total - high.astype(F32)).astype(BF16)
        for i in range(members):
            block = peers[first_k * members + i]
            rows = slice(i * capacity, (i + 1) * capacity)
            gained[0, block] = high[rows]
            gained[1, block] = low[rows]
    place_back = placing_t[...]
    for c in range(COLUMN_CHUNKS):
        span = slice(c * step, (c + 1) * step)
        high = gained[0, :, :, span].reshape(streams, step)
        low = gained[1, :, :, span].reshape(streams, step)
        out_ref[:, span] = (
            residual[:, span].astype(F32)
            + jnp.dot(place_back, high, preferred_element_type=F32)
            + jnp.dot(place_back, low, preferred_element_type=F32)
        ).astype(BF16)


def fused_body(residual, fresh_qkv, active, home_slot, kv_cache, lengths, w_out):
    n = lax.axis_size("dp")
    streams, columns = residual.shape
    width = fresh_qkv.shape[2]
    heads = width // HD
    capacity = streams // n
    row = (n, capacity, width + LANES)
    rows = streams // ROW_GROUPS
    vmem = pl.BlockSpec(memory_space=pltpu.VMEM)
    anywhere = pl.BlockSpec(memory_space=pl.ANY)
    dma = pltpu.SemaphoreType.DMA
    return pl.pallas_call(
        functools.partial(kernel, n, heads),
        out_shape=jax.ShapeDtypeStruct((streams, columns), BF16),
        in_specs=[vmem] * 4 + [anywhere] * 3,
        out_specs=vmem,
        scratch_shapes=[
            pltpu.VMEM(kv_cache.shape, BF16),
            pltpu.VMEM(w_out.shape, BF16),
            pltpu.VMEM(residual.shape, BF16),
            pltpu.VMEM(row, BF16),
            pltpu.VMEM(row, BF16),
            pltpu.VMEM(row, BF16),
            pltpu.VMEM(row, BF16),
            pltpu.VMEM((streams, width), BF16),
            pltpu.VMEM((n, capacity, LANES), F32),
            pltpu.VMEM((streams, LANES), F32),
            pltpu.VMEM((streams, streams), BF16),
            pltpu.VMEM((streams, width + LANES), BF16),
            pltpu.VMEM((streams, width), BF16),
            pltpu.VMEM((n, capacity, width), BF16),
            pltpu.VMEM((ROW_GROUPS, rows, width), BF16),
            pltpu.VMEM((ROW_GROUPS, rows, columns), BF16),
            pltpu.VMEM((ROW_GROUPS, rows, columns), BF16),
            pltpu.VMEM((ROW_GROUPS, rows, columns), F32),
            pltpu.VMEM((2, n, capacity, columns), BF16),
            dma((KV_PARTS,)),
            dma,
            dma,
            dma((n,)),
            dma((n,)),
            dma((n,)),
            dma((n,)),
            dma((ROW_GROUPS,)),
            dma((ROW_GROUPS,)),
        ],
        compiler_params=pltpu.CompilerParams(
            collective_id=0, has_side_effects=True, vmem_limit_bytes=60 * 1024 * 1024
        ),
    )(
        home_slot.reshape(1, streams),
        active.reshape(1, streams),
        lengths.reshape(1, streams),
        fresh_qkv.reshape(streams, 3 * width),
        kv_cache,
        w_out,
        residual,
    )


def body(residual, fresh_qkv, active, home_slot, kv_cache, lengths, w_out):
    n = lax.axis_size("dp")
    streams = home_slot.shape[0]
    fits = (
        lax.axis_size("tensor") == 2
        and n % ROW_GROUPS == 0
        and n & (n - 1) == 0
        and streams % n == 0
        and (streams // n) % 16 == 0
        and streams <= 256
        and streams & (streams - 1) == 0
    )
    chosen = fused_body if fits else general_body
    return chosen(residual, fresh_qkv, active, home_slot, kv_cache, lengths, w_out)


def solution(mesh):
    placed = (
        P("dp", "tensor"),
        P("dp", None, "tensor"),
        P("dp"),
        P("dp"),
        P("dp", None, None, "tensor"),
        P("dp"),
        P("tensor", None),
    )
    return jax.shard_map(
        body, mesh=mesh, in_specs=placed, out_specs=P("dp", "tensor"), check_vma=False
    )
```
